8 devices in a mesh: dp: 1 (over z), ep: 8 (over x, y, core).
Axes of the slice: x: 2, y: 2, z: 1, core: 2. Of those that a mesh axis runs over, the one named last changes fastest.
Arguments:
- x: bfloat16 [1, 8, 256, 3584], P('dp', 'ep')
- expert: int32 [1, 8, 256, 8], P('dp', 'ep')
- slot: int32 [1, 8, 256, 8], P('dp', 'ep')
- gate: float32 [1, 8, 256, 8], P('dp', 'ep')
- w_gate: bfloat16 [32, 3584, 2560], P('ep')
- w_up: bfloat16 [32, 3584, 2560], P('ep')
- w_down: bfloat16 [32, 2560, 3584], P('ep')
- s_gate: bfloat16 [3584, 20480], replicated
- s_up: bfloat16 [3584, 20480], replicated
- s_down: bfloat16 [20480, 3584], replicated
Outputs:
- y: bfloat16 [1, 8, 256, 3584], P('dp', 'ep')
All inputs are finite; a program needn't handle non-finite values.
Results may differ from the reference program's by a relative error of at most 0.009.
Values are sent between devices in bfloat16 or wider.
A program may use at most 2 GiB of HBM per device.

```python
import jax
import jax.numpy as jnp

MEMBERS = 8
TOKENS = 256
D = 3584
FF = 2560
TOP = 8
EXPERTS = 32
SHARED_FF = 20480
SLOTS = 5 * TOKENS * TOP // (4 * EXPERTS)


def setup_inputs(seed: int = 0, part: int = 0) -> dict:
    own, k1, k2, k3, k4, k5, k6 = jax.random.split(jax.random.key(seed), 7)
    kx, ke, kl, kg = jax.random.split(jax.random.fold_in(own, part), 4)
    devices = (1, MEMBERS)
    place = jax.random.permutation(kl, jnp.arange(EXPERTS, dtype=jnp.uint32))
    slow = ((EXPERTS + (9 * place) % EXPERTS) << ((9 * place) // EXPERTS)) // EXPERTS
    wait = (jax.random.bits(ke, (*devices, TOKENS, EXPERTS), jnp.uint32) >> 10) * slow
    expert = jnp.argsort(wait, axis=-1)[..., :TOP].astype(jnp.int32)
    chosen = jax.nn.one_hot(expert, EXPERTS, dtype=jnp.int32)
    in_line = jnp.cumsum(chosen.reshape(*devices, TOKENS * TOP, EXPERTS), axis=2) - 1
    slot = jnp.sum(in_line.reshape(chosen.shape) * chosen, axis=-1)

    def one(key, rows, columns):
        return (jax.random.normal(key, (rows, columns), jnp.float32) * rows**-0.5).astype(jnp.bfloat16)

    def weights(key, rows, columns):
        return jax.lax.map(lambda k: one(k, rows, columns), jax.random.split(key, EXPERTS))

    return {
        "x": jax.random.normal(kx, (*devices, TOKENS, D), jnp.float32).astype(jnp.bfloat16),
        "expert": expert,
        "slot": slot,
        "gate": jax.nn.softmax(jax.random.normal(kg, expert.shape, jnp.float32)),
        "w_gate": weights(k1, D, FF),
        "w_up": weights(k2, D, FF),
        "w_down": weights(k3, FF, D),
        "s_gate": one(k4, D, SHARED_FF),
        "s_up": one(k5, D, SHARED_FF),
        "s_down": one(k6, SHARED_FF, D),
    }


def einsum(form, a, b):
    return jnp.einsum(form, a.astype(jnp.float32), b.astype(jnp.float32))


def for_all(x, s_gate, s_up, s_down):
    h = jax.nn.silu(einsum("...d,df->...f", x, s_gate)) * einsum("...d,df->...f", x, s_up)
    return einsum("...f,fd->...d", h.astype(jnp.bfloat16), s_down)


def reference(x, expert, slot, gate, w_gate, w_up, w_down, s_gate, s_up, s_down):
    to_expert = jax.nn.one_hot(expert, EXPERTS, dtype=jnp.bfloat16)
    to_slot = jax.nn.one_hot(slot, SLOTS, dtype=jnp.bfloat16)
    weighted = to_expert * gate[..., None].astype(jnp.bfloat16)
    dispatch = einsum("abtke,abtkc->abtec", to_expert, to_slot).astype(jnp.bfloat16)
    combine = einsum("abtke,abtkc->abtec", weighted, to_slot).astype(jnp.bfloat16)
    z = einsum("abtec,abtd->aebcd", dispatch, x).astype(jnp.bfloat16)
    h = jax.nn.silu(einsum("aebcd,edf->aebcf", z, w_gate))
    h = (h * einsum("aebcd,edf->aebcf", z, w_up)).astype(jnp.bfloat16)
    out = einsum("aebcf,efd->aebcd", h, w_down).astype(jnp.bfloat16)
    y = einsum("abtec,aebcd->abtd", combine, out)
    return (y + for_all(x, s_gate, s_up, s_down)).astype(jnp.bfloat16)
```

```python
import functools

import jax
import jax.numpy as jnp
from jax import lax
from jax.experimental import pallas as pl
from jax.experimental.pallas import tpu as pltpu
from jax.sharding import PartitionSpec as P

CW = 512
WIN = 96
CWIN = 128
VMEM = 66_500_000


def silu_mul(g, u):
    return (g * jax.nn.sigmoid(g) * u).astype(jnp.bfloat16)


def dot(a, b):
    return jnp.dot(a, b, preferred_element_type=jnp.float32)


FLIPS = ((0, 0, 0), (0, 1, 0), (1, 0, 0), (1, 1, 0), (0, 0, 1), (0, 1, 1), (1, 0, 1), (1, 1, 1))
CHUNKS = 4
HALVES = 6
ROWS = 3072


def member(flip):
    me = lax.axis_index("ep")
    x, y, c = lax.div(me, 4), lax.rem(lax.div(me, 2), 2), lax.rem(me, 2)
    fx, fy, fc = flip
    return (x + fx * (1 - 2 * x)) * 4 + (y + fy * (1 - 2 * y)) * 2 + c + fc * (1 - 2 * c)


def greet():
    barrier = pltpu.get_barrier_semaphore()
    for flip in FLIPS[1:]:
        pl.semaphore_signal(
            barrier, inc=1, device_id={"ep": member(flip)}, device_id_type=pl.DeviceIdType.MESH
        )
    pl.semaphore_wait(barrier, len(FLIPS) - 1)


def remote(src, dst, ssem, rsem, to):
    return pltpu.make_async_remote_copy(
        src_ref=src, dst_ref=dst, send_sem=ssem, recv_sem=rsem,
        device_id={"ep": to}, device_id_type=pl.DeviceIdType.MESH,
    )


def start_all(copies):
    for c in copies:
        c.start()


def wait_all(copies):
    for c in copies:
        c.wait()


class Shared:
    def __init__(self, lo, tiles, x, sg, su, sd, h, wb, wsem):
        self.lo, self.tiles, self.nd = lo, tiles, x.shape[1] // CW
        self.x, self.sg, self.su, self.sd, self.h, self.wb, self.wsem = x, sg, su, sd, h, wb, wsem
        self.parts = tiles * CW // ROWS

    def up(self, i, slot):
        c = pl.ds(pl.multiple_of(self.lo + i * CW, CW), CW)
        return [
            pltpu.make_async_copy(w.at[:, c], self.wb.at[2 * slot + k], self.wsem.at[2 * slot + k])
            for k, w in enumerate((self.sg, self.su))
        ]

    def down(self, j, r, slot):
        c = pl.ds(pl.multiple_of(j * CW, CW), CW)
        return pltpu.make_async_copy(
            self.sd.at[pl.ds(self.lo + r * ROWS, ROWS), c], self.wb.at[slot, pl.ds(0, ROWS)], self.wsem.at[slot]
        )

    def begin(self):
        for i in range(HALVES // 2):
            start_all(self.up(i, i))

    def run(self, store, up_hooks, down_hooks):
        ring, tiles, nd, parts, h, wb = HALVES // 2, self.tiles, self.nd, self.parts, self.h, self.wb

        def up(i, _):
            slot = lax.rem(i, ring)
            wait_all(self.up(i, slot))
            g = dot(self.x[...], wb[2 * slot])
            u = dot(self.x[...], wb[2 * slot + 1])
            h[:, pl.ds(pl.multiple_of(i * CW, CW), CW)] = silu_mul(g, u)

            @pl.when(i + ring < tiles)
            def _():
                start_all(self.up(i + ring, slot))

            for k in range(ring):
                @pl.when(i == tiles - ring + k)
                def _():
                    for n in (2 * k, 2 * k + 1):
                        self.down(n // parts, n % parts, n).start()

            for at, fn in up_hooks:
                pl.when(i == at)(fn)
            return 0

        lax.fori_loop(0, tiles, up, 0)
        deep = HALVES // parts

        def down(j, _):
            base = lax.rem(j, deep) * parts
            o = None
            for r in range(parts):
                self.down(j, r, base + r).wait()
                d = dot(h[:, r * ROWS:(r + 1) * ROWS], wb[base + r, 0:ROWS, :])
                o = d if o is None else o + d
            store(pl.ds(pl.multiple_of(j * CW, CW), CW), o)

            @pl.when(j + deep < nd)
            def _():
                for r in range(parts):
                    self.down(j + deep, r, base + r).start()

            for at, fn in down_hooks:
                pl.when(j == at)(fn)
            return 0

        lax.fori_loop(0, nd, down, 0)


def first_kernel(lo, tiles, x, dense, sg, su, sd, out, x_all, w_all, h, wb, wsem, lsem, ssem, rsem, sw, rw):
    tokens = x.shape[0]
    core = lax.rem(lax.axis_index("ep"), 2)
    size = tokens // CHUNKS
    part = lambda k: pl.ds(k * size, size)
    work = Shared(lo, tiles, x, sg, su, sd, h, wb, wsem)
    work.begin()
    keep = [
        pltpu.make_async_copy(x, x_all.at[0], lsem.at[0]),
        pltpu.make_async_copy(dense, w_all.at[0], lsem.at[1]),
    ]
    start_all(keep)
    greet()

    own = lambda p, k: remote(
        x.at[part(k)], x_all.at[p, part(k)], ssem.at[p, k], rsem.at[p, k], member(FLIPS[p])
    )
    diag_to = (1 - core) * member(FLIPS[1]) + core * member(FLIPS[2])
    diag = lambda k: remote(
        x_all.at[2 - core, part(k)], x_all.at[3, part(k)], ssem.at[3, k], rsem.at[3, k], diag_to
    )
    mate = lambda p, k: remote(
        x_all.at[p, part(k)], x_all.at[p + 4, part(k)], ssem.at[p + 4, k], rsem.at[p + 4, k], member(FLIPS[4])
    )
    small = [
        remote(dense, w_all.at[p], sw.at[p], rw.at[p], member(FLIPS[p])) for p in range(1, len(FLIPS))
    ]
    start_all(small)
    for k in range(CHUNKS):
        own(1, k).start()
        own(2, k).start()
    for k in range(CHUNKS):
        own(4, k).start()

    def arrived(k):
        own(1, k).wait_recv()
        own(2, k).wait_recv()
        diag(k).start()
        mate(1, k).start()
        mate(2, k).start()

    def around(k):
        diag(k).wait_recv()
        mate(3, k).start()

    up_hooks = [(6, lambda: arrived(0)), (10, lambda: arrived(1)), (14, lambda: arrived(2))]
    down_hooks = [
        (0, lambda: arrived(3)), (2, lambda: around(0)), (4, lambda: around(1)), (5, lambda: around(2)),
        (6, lambda: around(3)),
    ]

    def store(c, o):
        out[:, c] = o

    work.run(store, up_hooks, down_hooks)
    wait_all(keep)
    wait_all(small)
    for k in range(CHUNKS):
        own(1, k).wait_send()
        own(2, k).wait_send()
        diag(k).wait_send()
        own(4, k).wait()
        for p in (1, 2, 3):
            mate(p, k).wait()


def last_kernel(lo, tiles, x, ya, yb, base, sg, su, sd, out, h, wb, acc, tv, rb, dg, rxy,
                wsem, lsem, ysem, ssem, rsem, s2, r2):
    tokens, d = x.shape
    f32, bf16 = jnp.float32, jnp.bfloat16
    core = lax.rem(lax.axis_index("ep"), 2)
    size = tokens // CHUNKS
    part = lambda k: pl.ds(k * size, size)
    work = Shared(lo, tiles, x, sg, su, sd, h, wb, wsem)
    order = (3, 1, 2, 0)
    load = lambda p, k: pltpu.make_async_copy(ya.at[p, part(k)], tv.at[p, part(k)], ysem.at[p, k])
    for k in range(CHUNKS):
        load(3, k).start()
    work.begin()
    for p in order[1:]:
        for k in range(CHUNKS):
            load(p, k).start()
    basecopy = pltpu.make_async_copy(base, acc, lsem.at[0])
    basecopy.start()
    greet()

    swap = lambda p, k: remote(
        yb.at[p, part(k)], rb.at[p, part(k)], ssem.at[p, k], rsem.at[p, k], member(FLIPS[4])
    )
    for p in order:
        for k in range(CHUNKS):
            swap(p, k).start()

    to_y, to_x = member(FLIPS[1]), member(FLIPS[2])
    near = (1 - core) * to_x + core * to_y
    relay = (1 - core) * to_y + core * to_x
    direct, turned = 2 - core, 1 + core
    send0 = lambda k: remote(tv.at[3, part(k)], dg.at[part(k)], s2.at[0, k], r2.at[0, k], near)
    send1 = lambda k: remote(
        tv.at[direct, part(k)], rxy.at[direct - 1, part(k)], s2.at[direct, k], r2.at[direct, k], near
    )
    send2 = lambda k: remote(
        tv.at[turned, part(k)], rxy.at[turned - 1, part(k)], s2.at[turned, k], r2.at[turned, k], relay
    )

    def far(k):
        load(3, k).wait()
        swap(3, k).wait_recv()
        tv[3, part(k)] = (tv[3, part(k)].astype(f32) + rb[3, part(k)].astype(f32)).astype(bf16)
        send0(k).start()

    def straight(k):
        load(direct, k).wait()
        swap(direct, k).wait_recv()
        tv[direct, part(k)] = (tv[direct, part(k)].astype(f32) + rb[direct, part(k)].astype(f32)).astype(bf16)
        send1(k).start()

    def passed(k):
        load(turned, k).wait()
        swap(turned, k).wait_recv()
        send0(k).wait_recv()
        tv[turned, part(k)] = (
            tv[turned, part(k)].astype(f32) + rb[turned, part(k)].astype(f32) + dg[part(k)].astype(f32)
        ).astype(bf16)
        send2(k).start()

    def both(fn, *ks):
        def run():
            for k in ks:
                fn(k)
        return run

    up_hooks = [
        (0, both(far, 0, 1, 2, 3)), (2, both(straight, 0, 1, 2, 3)),
        (4, both(passed, 0)), (6, both(passed, 1)), (8, both(passed, 2)), (10, both(passed, 3)),
        (11, basecopy.wait),
    ]

    def store(c, o):
        acc[:, c] = acc[:, c] + o

    work.run(store, up_hooks, [])
    for k in range(CHUNKS):
        load(0, k).wait()
        swap(0, k).wait_recv()
        for q in (1, 2):
            remote(tv.at[q, part(k)], rxy.at[q - 1, part(k)], s2.at[q, k], r2.at[q, k], to_y).wait_recv()

        def rows(i, _, k=k):
            r = pl.ds(pl.multiple_of(k * size + i * 16, 16), 16)
            out[r, :] = (
                acc[r, :] + tv[0, r, :].astype(f32) + rb[0, r, :].astype(f32)
                + rxy[0, r, :].astype(f32) + rxy[1, r, :].astype(f32)
            ).astype(bf16)
            return 0

        lax.fori_loop(0, size // 16, rows, 0)
    for k in range(CHUNKS):
        for p in range(4):
            swap(p, k).wait_send()
        send0(k).wait_send()
        send1(k).wait_send()
        send2(k).wait_send()


ANY = pl.BlockSpec(memory_space=pl.ANY)
VM = pl.BlockSpec(memory_space=pltpu.VMEM)


def shared_cost(tokens, d, width):
    return pl.CostEstimate(
        flops=6 * tokens * d * width, bytes_accessed=6 * d * width, transcendentals=tokens * width
    )


def first(x, dense, sg, su, sd, lo, tiles):
    tokens, d = x.shape
    n = len(FLIPS)
    dma = pltpu.SemaphoreType.DMA
    return pl.pallas_call(
        functools.partial(first_kernel, lo, tiles),
        out_shape=(
            jax.ShapeDtypeStruct((tokens, d), jnp.float32),
            jax.ShapeDtypeStruct((n, tokens, d), x.dtype),
            jax.ShapeDtypeStruct((n, *dense.shape), dense.dtype),
        ),
        in_specs=[VM, VM, ANY, ANY, ANY],
        out_specs=(VM, ANY, ANY),
        scratch_shapes=[
            pltpu.VMEM((tokens, tiles * CW), jnp.bfloat16),
            pltpu.VMEM((HALVES, d, CW), jnp.bfloat16),
            dma((HALVES,)), dma((2,)), dma((n, CHUNKS)), dma((n, CHUNKS)), dma((n,)), dma((n,)),
        ],
        compiler_params=pltpu.CompilerParams(vmem_limit_bytes=VMEM, collective_id=0, has_side_effects=True),
        cost_estimate=shared_cost(tokens, d, tiles * CW),
        name="first",
    )(x, dense, sg, su, sd)


def last(x, ya, yb, base, sg, su, sd, lo, tiles):
    tokens, d = x.shape
    dma = pltpu.SemaphoreType.DMA
    bf16 = jnp.bfloat16
    return pl.pallas_call(
        functools.partial(last_kernel, lo, tiles),
        out_shape=jax.ShapeDtypeStruct((tokens, d), bf16),
        in_specs=[VM, ANY, ANY, ANY, ANY, ANY, ANY],
        out_specs=VM,
        scratch_shapes=[
            pltpu.VMEM((tokens, tiles * CW), bf16),
            pltpu.VMEM((HALVES, d, CW), bf16),
            pltpu.VMEM((tokens, d), jnp.float32),
            pltpu.VMEM((4, tokens, d), bf16),
            pltpu.VMEM((4, tokens, d), bf16),
            pltpu.VMEM((tokens, d), bf16),
            pltpu.VMEM((2, tokens, d), bf16),
            dma((HALVES,)), dma((1,)), dma((4, CHUNKS)), dma((4, CHUNKS)), dma((4, CHUNKS)),
            dma((3, CHUNKS)), dma((3, CHUNKS)),
        ],
        compiler_params=pltpu.CompilerParams(vmem_limit_bytes=VMEM, collective_id=1, has_side_effects=True),
        cost_estimate=shared_cost(tokens, d, tiles * CW),
        name="last",
    )(x, ya, yb, base, sg, su, sd)


UNITS = 4
UW = 256
UNIT_COST = 104
LEAST_COST = 960


def routed_kernel(lo, units, x_hbm, wt_ref, wg, wu, wd, sg, su, sd, ya, yb_hbm, z, h, wb, yb, hm, cmat,
                  pos_v, off_v, off_s, wsem, xsem, ysem, osem, usem):
    ne, d, ff = wg.shape
    members, tokens = x_hbm.shape[:2]
    nf, nd = ff // CW, d // CW
    gitems, ditems = nf * ne, nd * ne
    ring = 3
    f32, bf16, i32 = jnp.float32, jnp.bfloat16, jnp.int32

    def gcopy(i, slot):
        e, f = lax.rem(i, ne), lax.div(i, ne)
        c = pl.ds(pl.multiple_of(f * CW, CW), CW)
        return [
            pltpu.make_async_copy(w.at[e, :, c], wb.at[2 * slot + k], wsem.at[2 * slot + k])
            for k, w in enumerate((wg, wu))
        ]

    def dcopy(i, slot):
        e, f = lax.rem(i, ne), lax.div(i, ne)
        c = pl.ds(pl.multiple_of(f * CW, CW), CW)
        return [pltpu.make_async_copy(wd.at[e, :, c], wb.at[slot, pl.ds(0, ff)], wsem.at[slot])]

    def xcopy(s, b):
        return [
            pltpu.make_async_copy(x_hbm.at[s, :, pl.ds(c * CW, CW)], yb.at[b, c], xsem.at[b, c])
            for c in range(nd)
        ]

    def start(copies):
        for c in copies:
            c.start()

    def wait(copies):
        for c in copies:
            c.wait()

    start(xcopy(0, 0))
    start(xcopy(1, 1))
    start(gcopy(0, 0))

    rows = members * ne
    me = lax.axis_index("ep")
    w = jnp.concatenate([wt_ref[s, me] for s in range(members)], axis=0)
    mask = w != 0.0
    mb = jnp.where(mask, 1.0, 0.0).astype(bf16)
    a0 = lax.broadcasted_iota(i32, (tokens, tokens), 0)
    a1 = lax.broadcasted_iota(i32, (tokens, tokens), 1)
    rank = dot(mb, jnp.where(a0 <= a1, 1.0, 0.0).astype(bf16))
    b0 = lax.broadcasted_iota(i32, (rows, rows), 0)
    b1 = lax.broadcasted_iota(i32, (rows, rows), 1)
    earlier = (lax.rem(b0, ne) == lax.rem(b1, ne)) & (b1 < b0)
    before = jnp.sum(dot(jnp.where(earlier, 1.0, 0.0).astype(bf16), mb), axis=1, keepdims=True)
    count = jnp.sum(jnp.where(mask, 1.0, 0.0), axis=1, keepdims=True)
    pos = jnp.where(mask, before + rank - 1.0, -1.0)
    for s in range(members):
        pos_v[s, 0:ne, :] = pos[s * ne:(s + 1) * ne]
    lane = lax.broadcasted_iota(i32, (rows, 128), 1)
    total = jnp.zeros((rows, tokens), f32)
    for s in range(members):
        every = jnp.concatenate([wt_ref[s, m] for m in range(members)], axis=0)
        total += jnp.where(every != 0.0, 1.0, 0.0)
    total = jnp.sum(total, axis=1, keepdims=True)
    off_v[...] = jnp.where(lane == 0, before, jnp.where(lane == 1, before + count, total)).astype(i32)
    cp = pltpu.make_async_copy(off_v, off_s, osem)
    cp.start()
    zero = jnp.zeros((16, d), bf16)

    def clear(i, _):
        for e in range(ne):
            z[e, pl.ds(pl.multiple_of(i * 16, 16), 16), :] = zero
        return 0

    lax.fori_loop(0, z.shape[1] // 16, clear, 0)
    cp.wait()

    costs = []
    for m in range(members):
        c = 0
        for e in range(ne):
            c += lax.div(off_s[m * ne + e, 2] + 127, 128) * 128
        costs.append(jnp.maximum(c, LEAST_COST))

    def give(_, carry):
        cost, held = carry
        best, who = jnp.where(held[0] < UNITS, cost[0], 1 << 20), 0
        for m in range(1, members):
            c = jnp.where(held[m] < UNITS, cost[m], 1 << 20)
            who = jnp.where(c < best, m, who)
            best = jnp.minimum(c, best)
        return (
            [jnp.where(who == m, cost[m] + UNIT_COST, cost[m]) for m in range(members)],
            [jnp.where(who == m, held[m] + 1, held[m]) for m in range(members)],
        )

    _, held = lax.fori_loop(0, units, give, (costs, [jnp.int32(0)] * members))
    first_unit, mine = 0, 0
    for m in range(members):
        first_unit += jnp.where(m < me, held[m], 0)
        mine += jnp.where(m == me, held[m], 0)

    def unit_col(u):
        return pl.multiple_of(lo + lax.div(first_unit + u, 2) * UW, UW)

    def ucopy(u):
        return [
            pltpu.make_async_copy(
                w.at[:, pl.ds(unit_col(u), UW)], wb.at[2 + u, :, pl.ds(k * UW, UW)], usem.at[u, k]
            )
            for k, w in enumerate((sg, su))
        ]

    def vcopy(u, q, par):
        c = pl.ds(pl.multiple_of(q * CW, CW), CW)
        return pltpu.make_async_copy(
            sd.at[pl.ds(unit_col(u), UW), c],
            z.at[u, pl.ds(0, UW), pl.ds(pl.multiple_of((2 + par) * CW, CW), CW)],
            usem.at[u, par],
        )

    def for_units(fn):
        for u in range(UNITS):
            @pl.when(u < mine)
            def _():
                fn(u)

    for_units(lambda u: start(ucopy(u)))
    odd = lax.rem(first_unit + me, 2)

    def units_of(half):
        u0 = lax.rem(odd + half, 2)
        return u0, jnp.maximum(lax.div(mine - u0 + 1, 2), 0)

    def window(s, e):
        st = off_s[s * ne + e, 0]
        return pl.multiple_of(lax.div(st, 16) * 16, 16)

    both = jnp.concatenate([pos, w, jnp.zeros((128 - 2 * rows, tokens), f32)], axis=0).T
    cl = lax.broadcasted_iota(i32, (tokens, CWIN), 1)
    for s in range(members):
        for e in range(ne):
            k = s * ne + e
            rel = both[:, k:k + 1].astype(i32) - window(s, e)
            cmat[s, :, e * CWIN:(e + 1) * CWIN] = jnp.where(
                rel == cl, both[:, rows + k:rows + k + 1], 0.0
            ).astype(bf16)

    wl = lax.broadcasted_iota(i32, (WIN, tokens), 0)

    def dispatch(s, _):
        b = lax.rem(s, 2)
        wait(xcopy(s, b))
        w0 = [window(s, e) for e in range(ne)]
        oh = jnp.concatenate([
            jnp.where(pos_v[s, e:e + 1, :].astype(i32) - w0[e] == wl, 1.0, 0.0).astype(bf16)
            for e in range(ne)
        ], axis=0)
        for c in range(nd):
            got = dot(oh, yb[b, c]).astype(bf16)
            for e in range(ne):
                at = (e, pl.ds(w0[e], WIN), slice(c * CW, (c + 1) * CW))
                z[at] = z[at] + got[e * WIN:(e + 1) * WIN]

        u0, nu = units_of(lax.div(s, 4))

        def unit(k, _):
            u = u0 + 2 * k
            @pl.when(lax.rem(s, 4) == 0)
            def _():
                wait(ucopy(u))

            xs = jnp.concatenate([yb[b, c] for c in range(nd)], axis=1)
            gu = dot(xs, wb[2 + u])
            hm[u, lax.rem(s, 4)] = silu_mul(gu[:, :UW], gu[:, UW:])
            return 0

        lax.fori_loop(0, nu, unit, 0)

        @pl.when(s + 2 < members)
        def _():
            start(xcopy(s + 2, b))

        return 0

    lax.fori_loop(0, members, dispatch, 0)
    for i in range(1, ring):
        start(gcopy(i, i))

    def tiles(e, body):
        n = off_s[(members - 1) * ne + e, 1]
        full = lax.div(n + 127, 256)
        lax.fori_loop(0, full, lambda m, c: (body(pl.multiple_of(m * 256, 256), 256), c)[1], 0)

        @pl.when(n > full * 256)
        def _():
            body(pl.multiple_of(full * 256, 256), 128)

    def gstep(i, _):
        e, f = lax.rem(i, ne), lax.div(i, ne)
        slot = lax.rem(i, ring)
        wait(gcopy(i, slot))
        c = pl.ds(pl.multiple_of(f * CW, CW), CW)

        def body(m, size):
            zt = z[e, pl.ds(m, size), :]
            g = dot(zt, wb[2 * slot])
            u = dot(zt, wb[2 * slot + 1])
            h[e, pl.ds(m, size), c] = silu_mul(g, u)

        tiles(e, body)

        @pl.when(i + ring < gitems)
        def _():
            start(gcopy(i + ring, slot))

        return 0

    lax.fori_loop(0, gitems, gstep, 0)

    for i in range(2 * ring):
        start(dcopy(i, i))

    def ycopy(q, par):
        c = pl.ds(pl.multiple_of(q * CW, CW), CW)
        half = members // 2
        return [
            pltpu.make_async_copy(yb.at[par, pl.ds(k * half, half)], y.at[:, :, c], ysem.at[par, k])
            for k, y in enumerate((ya, yb_hbm))
        ]

    for_units(lambda u: vcopy(u, 0, 0).start())

    def dpair(q, _):
        par = lax.rem(q, 2)

        @pl.when(q + 1 < nd)
        def _():
            for_units(lambda u: vcopy(u, q + 1, 1 - par).start())

        oc = pl.ds(pl.multiple_of(par * CW, CW), CW)

        def estep(e, _):
            i = q * ne + e
            slot = lax.rem(i, 2 * ring)
            wait(dcopy(i, slot))

            def body(m, size):
                o = dot(h[e, pl.ds(m, size), :], wb[slot, 0:ff, :])
                z[e, pl.ds(m, size), oc] = o.astype(bf16)

            tiles(e, body)

            @pl.when(i + 2 * ring < ditems)
            def _():
                start(dcopy(i + 2 * ring, slot))

            return 0

        lax.fori_loop(0, ne, estep, 0)

        @pl.when(q >= 2)
        def _():
            wait(ycopy(q - 2, par))

        for_units(lambda u: vcopy(u, q, par).wait())
        vc = pl.ds(pl.multiple_of((2 + par) * CW, CW), CW)

        def two(k, _):
            u0, nu = units_of(lax.div(k, 2))
            for n in range(UNITS // 2 + 1):
                @pl.when(nu == n)
                def _():
                    for j in range(2):
                        s = 2 * k + j
                        left = [cmat[s]] + [hm[u0 + 2 * i, lax.rem(s, 4)] for i in range(n)]
                        right = [z[e, pl.ds(window(s, e), CWIN), oc] for e in range(ne)]
                        right += [z[u0 + 2 * i, 0:UW, vc] for i in range(n)]
                        yb[par, s] = dot(
                            jnp.concatenate(left, axis=1), jnp.concatenate(right, axis=0)
                        ).astype(bf16)
            return 0

        lax.fori_loop(0, members // 2, two, 0)
        start(ycopy(q, par))
        return 0

    lax.fori_loop(0, nd, dpair, 0)
    wait(ycopy(nd - 2, (nd - 2) % 2))
    wait(ycopy(nd - 1, (nd - 1) % 2))


def routed(x_all, wt, wg, wu, wd, sg, su, sd, lo, width):
    members, tokens, d = x_all.shape
    ne, _, ff = wg.shape
    rows = members * 80
    anyspec = pl.BlockSpec(memory_space=pl.ANY)
    vspec = pl.BlockSpec(memory_space=pltpu.VMEM)
    half = jax.ShapeDtypeStruct((members // 2, tokens, d), jnp.bfloat16)
    return pl.pallas_call(
        functools.partial(routed_kernel, lo, 2 * width // UW),
        out_shape=(half, half),
        in_specs=[anyspec, vspec] + [anyspec] * 6,
        out_specs=(anyspec, anyspec),
        scratch_shapes=[
            pltpu.VMEM((ne, rows + 48, d), jnp.bfloat16),
            pltpu.VMEM((ne, rows, ff), jnp.bfloat16),
            pltpu.VMEM((6, d, CW), jnp.bfloat16),
            pltpu.VMEM((2, members, tokens, CW), jnp.bfloat16),
            pltpu.VMEM((UNITS, 4, tokens, UW), jnp.bfloat16),
            pltpu.VMEM((members, tokens, ne * CWIN), jnp.bfloat16),
            pltpu.VMEM((members, 8, tokens), jnp.float32),
            pltpu.VMEM((members * ne, 128), jnp.int32),
            pltpu.SMEM((members * ne, 128), jnp.int32),
            pltpu.SemaphoreType.DMA((6,)),
            pltpu.SemaphoreType.DMA((2, d // CW)),
            pltpu.SemaphoreType.DMA((2, 2)),
            pltpu.SemaphoreType.DMA,
            pltpu.SemaphoreType.DMA((UNITS, 2)),
        ],
        compiler_params=pltpu.CompilerParams(vmem_limit_bytes=VMEM),
        cost_estimate=pl.CostEstimate(
            flops=6 * 1600 * d * ff, bytes_accessed=6 * ne * d * ff, transcendentals=1600 * ff
        ),
        name="routed",
    )(x_all, wt, wg, wu, wd, sg, su, sd)


def solution(mesh):
    members = mesh.shape["ep"]

    def body(x, expert, slot, gate, wg, wu, wd, sg, su, sd):
        tokens, top = expert.shape[2:]
        experts = wg.shape[0] * members
        slots = 5 * tokens * top // (4 * experts)
        x2 = x.reshape(tokens, x.shape[-1])
        f32, bf16 = jnp.float32, jnp.bfloat16

        g = jnp.where(slot < slots, gate.astype(bf16).astype(f32), 0.0).reshape(tokens, top)
        ids = expert.reshape(tokens, top)
        dense = jnp.sum(
            jnp.where(ids.T[:, None, :] == jnp.arange(experts)[None, :, None], g.T[:, None, :], 0.0), axis=0
        )
        acc, x_all, w_all = first(x2, dense, sg, su, sd, 0, 18)
        ya, yb = routed(x_all, w_all.reshape(members, members, -1, tokens), wg, wu, wd, sg, su, sd, 18 * CW, 4 * CW)
        y = last(x2, ya, yb, acc, sg, su, sd, 22 * CW, 18)
        return y.reshape(x.shape)

    a = P("dp", "ep", None, None)
    w = P("ep", None, None)
    s = P(None, None)
    return jax.shard_map(
        body, mesh=mesh, in_specs=(a, a, a, a, w, w, w, s, s, s), out_specs=a, check_vma=False
    )
```

```python
import functools

import jax
import jax.numpy as jnp
from jax import lax
from jax.experimental import pallas as pl
from jax.experimental.pallas import tpu as pltpu
from jax.sharding import PartitionSpec as P

CW = 512
WIN = 96
CWIN = 128
VMEM = 67_043_328


def silu_mul(g, u):
    return (g * jax.nn.sigmoid(g) * u).astype(jnp.bfloat16)


def dot(a, b):
    return jnp.dot(a, b, preferred_element_type=jnp.float32)


FLIPS = ((0, 0, 0), (0, 1, 0), (1, 0, 0), (1, 1, 0), (0, 0, 1), (0, 1, 1), (1, 0, 1), (1, 1, 1))
CHUNKS = 4
EDGE = 18
HALVES = 6
ROWS = 3072


def member(flip):
    me = lax.axis_index("ep")
    x, y, c = lax.div(me, 4), lax.rem(lax.div(me, 2), 2), lax.rem(me, 2)
    fx, fy, fc = flip
    return (x + fx * (1 - 2 * x)) * 4 + (y + fy * (1 - 2 * y)) * 2 + c + fc * (1 - 2 * c)


def greet():
    barrier = pltpu.get_barrier_semaphore()
    for flip in FLIPS[1:]:
        pl.semaphore_signal(
            barrier, inc=1, device_id={"ep": member(flip)}, device_id_type=pl.DeviceIdType.MESH
        )
    pl.semaphore_wait(barrier, len(FLIPS) - 1)


def remote(src, dst, ssem, rsem, to):
    return pltpu.make_async_remote_copy(
        src_ref=src, dst_ref=dst, send_sem=ssem, recv_sem=rsem,
        device_id={"ep": to}, device_id_type=pl.DeviceIdType.MESH,
    )


def start_all(copies):
    for c in copies:
        c.start()


def wait_all(copies):
    for c in copies:
        c.wait()


class Shared:
    def __init__(self, lo, tiles, x, sg, su, sd, h, wb, wsem):
        self.lo, self.tiles, self.nd = lo, tiles, x.shape[1] // CW
        self.x, self.sg, self.su, self.sd, self.h, self.wb, self.wsem = x, sg, su, sd, h, wb, wsem
        self.parts = tiles * CW // ROWS

    def up(self, i, slot):
        c = pl.ds(pl.multiple_of(self.lo + i * CW, CW), CW)
        return [
            pltpu.make_async_copy(w.at[:, c], self.wb.at[2 * slot + k], self.wsem.at[2 * slot + k])
            for k, w in enumerate((self.sg, self.su))
        ]

    def down(self, j, r, slot):
        c = pl.ds(pl.multiple_of(j * CW, CW), CW)
        return pltpu.make_async_copy(
            self.sd.at[pl.ds(self.lo + r * ROWS, ROWS), c], self.wb.at[slot, pl.ds(0, ROWS)], self.wsem.at[slot]
        )

    def begin(self):
        for i in range(HALVES // 2):
            start_all(self.up(i, i))

    def run(self, store, up_hooks, down_hooks):
        ring, tiles, nd, parts, h, wb = HALVES // 2, self.tiles, self.nd, self.parts, self.h, self.wb

        def up(i, _):
            slot = lax.rem(i, ring)
            wait_all(self.up(i, slot))
            g = dot(self.x[...], wb[2 * slot])
            u = dot(self.x[...], wb[2 * slot + 1])
            h[:, pl.ds(pl.multiple_of(i * CW, CW), CW)] = silu_mul(g, u)

            @pl.when(i + ring < tiles)
            def _():
                start_all(self.up(i + ring, slot))

            for k in range(ring):
                @pl.when(i == tiles - ring + k)
                def _():
                    for n in (2 * k, 2 * k + 1):
                        self.down(n // parts, n % parts, n).start()

            for at, fn in up_hooks:
                pl.when(i == at)(fn)
            return 0

        lax.fori_loop(0, tiles, up, 0)
        deep = HALVES // parts

        def down(j, _):
            base = lax.rem(j, deep) * parts
            o = None
            for r in range(parts):
                self.down(j, r, base + r).wait()
                d = dot(h[:, r * ROWS:(r + 1) * ROWS], wb[base + r, 0:ROWS, :])
                o = d if o is None else o + d
            store(pl.ds(pl.multiple_of(j * CW, CW), CW), o)

            @pl.when(j + deep < nd)
            def _():
                for r in range(parts):
                    self.down(j + deep, r, base + r).start()

            for at, fn in down_hooks:
                pl.when(j == at)(fn)
            return 0

        lax.fori_loop(0, nd, down, 0)


def first_kernel(lo, tiles, x, dense, sg, su, sd, out, x_all, w_all, h, wb, wsem, lsem, ssem, rsem, sw, rw):
    tokens = x.shape[0]
    core = lax.rem(lax.axis_index("ep"), 2)
    size = tokens // CHUNKS
    part = lambda k: pl.ds(k * size, size)
    work = Shared(lo, tiles, x, sg, su, sd, h, wb, wsem)
    work.begin()
    keep = [
        pltpu.make_async_copy(x, x_all.at[0], lsem.at[0]),
        pltpu.make_async_copy(dense, w_all.at[0], lsem.at[1]),
    ]
    start_all(keep)
    greet()

    own = lambda p, k: remote(
        x.at[part(k)], x_all.at[p, part(k)], ssem.at[p, k], rsem.at[p, k], member(FLIPS[p])
    )
    diag_to = (1 - core) * member(FLIPS[1]) + core * member(FLIPS[2])
    diag = lambda k: remote(
        x_all.at[2 - core, part(k)], x_all.at[3, part(k)], ssem.at[3, k], rsem.at[3, k], diag_to
    )
    mate = lambda p, k: remote(
        x_all.at[p, part(k)], x_all.at[p + 4, part(k)], ssem.at[p + 4, k], rsem.at[p + 4, k], member(FLIPS[4])
    )
    small = [
        remote(dense, w_all.at[p], sw.at[p], rw.at[p], member(FLIPS[p])) for p in range(1, len(FLIPS))
    ]
    start_all(small)
    for k in range(CHUNKS):
        own(1, k).start()
        own(2, k).start()
    for k in range(CHUNKS):
        own(4, k).start()

    def arrived(k):
        own(1, k).wait_recv()
        own(2, k).wait_recv()
        diag(k).start()
        mate(1, k).start()
        mate(2, k).start()

    def around(k):
        diag(k).wait_recv()
        mate(3, k).start()

    up_hooks = [(4, lambda: arrived(0)), (8, lambda: arrived(1)), (12, lambda: arrived(2)), (16, lambda: arrived(3))]
    down_hooks = [
        (2, lambda: around(0)), (4, lambda: around(1)), (5, lambda: around(2)), (6, lambda: around(3)),
    ]

    def store(c, o):
        out[:, c] = o

    work.run(store, up_hooks, down_hooks)
    wait_all(keep)
    wait_all(small)
    for k in range(CHUNKS):
        own(1, k).wait_send()
        own(2, k).wait_send()
        diag(k).wait_send()
        own(4, k).wait()
        for p in (1, 2, 3):
            mate(p, k).wait()


def last_kernel(lo, tiles, x, ya, yb, base, sg, su, sd, out, h, wb, acc, tv, rb, dg, rxy,
                wsem, lsem, ysem, ssem, rsem, s2, r2):
    tokens, d = x.shape
    f32, bf16 = jnp.float32, jnp.bfloat16
    core = lax.rem(lax.axis_index("ep"), 2)
    size = tokens // CHUNKS
    part = lambda k: pl.ds(k * size, size)
    work = Shared(lo, tiles, x, sg, su, sd, h, wb, wsem)
    order = (3, 1, 2, 0)
    load = lambda p, k: pltpu.make_async_copy(ya.at[p, part(k)], tv.at[p, part(k)], ysem.at[p, k])
    for k in range(CHUNKS):
        load(3, k).start()
    work.begin()
    for p in order[1:]:
        for k in range(CHUNKS):
            load(p, k).start()
    basecopy = pltpu.make_async_copy(base, acc, lsem.at[0])
    basecopy.start()
    greet()

    swap = lambda p, k: remote(
        yb.at[p, part(k)], rb.at[p, part(k)], ssem.at[p, k], rsem.at[p, k], member(FLIPS[4])
    )
    for p in order:
        for k in range(CHUNKS):
            swap(p, k).start()

    to_y, to_x = member(FLIPS[1]), member(FLIPS[2])
    near = (1 - core) * to_x + core * to_y
    relay = (1 - core) * to_y + core * to_x
    direct, turned = 2 - core, 1 + core
    send0 = lambda k: remote(tv.at[3, part(k)], dg.at[part(k)], s2.at[0, k], r2.at[0, k], near)
    send1 = lambda k: remote(
        tv.at[direct, part(k)], rxy.at[direct - 1, part(k)], s2.at[direct, k], r2.at[direct, k], near
    )
    send2 = lambda k: remote(
        tv.at[turned, part(k)], rxy.at[turned - 1, part(k)], s2.at[turned, k], r2.at[turned, k], relay
    )

    def far(k):
        load(3, k).wait()
        swap(3, k).wait_recv()
        tv[3, part(k)] = (tv[3, part(k)].astype(f32) + rb[3, part(k)].astype(f32)).astype(bf16)
        send0(k).start()

    def straight(k):
        load(direct, k).wait()
        swap(direct, k).wait_recv()
        tv[direct, part(k)] = (tv[direct, part(k)].astype(f32) + rb[direct, part(k)].astype(f32)).astype(bf16)
        send1(k).start()

    def passed(k):
        load(turned, k).wait()
        swap(turned, k).wait_recv()
        send0(k).wait_recv()
        tv[turned, part(k)] = (
            tv[turned, part(k)].astype(f32) + rb[turned, part(k)].astype(f32) + dg[part(k)].astype(f32)
        ).astype(bf16)
        send2(k).start()

    def both(fn, *ks):
        def run():
            for k in ks:
                fn(k)
        return run

    both(far, 0, 1, 2, 3)()
    up_hooks = [
        (0, both(straight, 0, 1, 2, 3)), (3, both(passed, 0)), (5, both(passed, 1)), (7, both(passed, 2)),
        (9, both(passed, 3)), (11, basecopy.wait),
    ]

    def store(c, o):
        acc[:, c] = acc[:, c] + o

    work.run(store, up_hooks, [])
    for k in range(CHUNKS):
        load(0, k).wait()
        swap(0, k).wait_recv()
        for q in (1, 2):
            remote(tv.at[q, part(k)], rxy.at[q - 1, part(k)], s2.at[q, k], r2.at[q, k], to_y).wait_recv()

        def rows(i, _, k=k):
            r = pl.ds(pl.multiple_of(k * size + i * 16, 16), 16)
            out[r, :] = (
                acc[r, :] + tv[0, r, :].astype(f32) + rb[0, r, :].astype(f32)
                + rxy[0, r, :].astype(f32) + rxy[1, r, :].astype(f32)
            ).astype(bf16)
            return 0

        lax.fori_loop(0, size // 16, rows, 0)
    for k in range(CHUNKS):
        for p in range(4):
            swap(p, k).wait_send()
        send0(k).wait_send()
        send1(k).wait_send()
        send2(k).wait_send()


ANY = pl.BlockSpec(memory_space=pl.ANY)
VM = pl.BlockSpec(memory_space=pltpu.VMEM)


def shared_cost(tokens, d, width):
    return pl.CostEstimate(
        flops=6 * tokens * d * width, bytes_accessed=6 * d * width, transcendentals=tokens * width
    )


def first(x, dense, sg, su, sd, lo, tiles):
    tokens, d = x.shape
    n = len(FLIPS)
    dma = pltpu.SemaphoreType.DMA
    return pl.pallas_call(
        functools.partial(first_kernel, lo, tiles),
        out_shape=(
            jax.ShapeDtypeStruct((tokens, d), jnp.float32),
            jax.ShapeDtypeStruct((n, tokens, d), x.dtype),
            jax.ShapeDtypeStruct((n, *dense.shape), dense.dtype),
        ),
        in_specs=[VM, VM, ANY, ANY, ANY],
        out_specs=(VM, ANY, ANY),
        scratch_shapes=[
            pltpu.VMEM((tokens, tiles * CW), jnp.bfloat16),
            pltpu.VMEM((HALVES, d, CW), jnp.bfloat16),
            dma((HALVES,)), dma((2,)), dma((n, CHUNKS)), dma((n, CHUNKS)), dma((n,)), dma((n,)),
        ],
        compiler_params=pltpu.CompilerParams(vmem_limit_bytes=VMEM, collective_id=0, has_side_effects=True),
        cost_estimate=shared_cost(tokens, d, tiles * CW),
        name="first",
    )(x, dense, sg, su, sd)


def last(x, ya, yb, base, sg, su, sd, lo, tiles):
    tokens, d = x.shape
    dma = pltpu.SemaphoreType.DMA
    bf16 = jnp.bfloat16
    return pl.pallas_call(
        functools.partial(last_kernel, lo, tiles),
        out_shape=jax.ShapeDtypeStruct((tokens, d), bf16),
        in_specs=[VM, ANY, ANY, ANY, ANY, ANY, ANY],
        out_specs=VM,
        scratch_shapes=[
            pltpu.VMEM((tokens, tiles * CW), bf16),
            pltpu.VMEM((HALVES, d, CW), bf16),
            pltpu.VMEM((tokens, d), jnp.float32),
            pltpu.VMEM((4, tokens, d), bf16),
            pltpu.VMEM((4, tokens, d), bf16),
            pltpu.VMEM((tokens, d), bf16),
            pltpu.VMEM((2, tokens, d), bf16),
            dma((HALVES,)), dma((1,)), dma((4, CHUNKS)), dma((4, CHUNKS)), dma((4, CHUNKS)),
            dma((3, CHUNKS)), dma((3, CHUNKS)),
        ],
        compiler_params=pltpu.CompilerParams(vmem_limit_bytes=VMEM, collective_id=1, has_side_effects=True),
        cost_estimate=shared_cost(tokens, d, tiles * CW),
        name="last",
    )(x, ya, yb, base, sg, su, sd)


UNITS = 5
BLOCKS = 3
UW = 256
UNIT_COST = 140
LEAST_COST = 880


def routed_kernel(lo, units, x_hbm, wt_ref, wg, wu, wd, sg, su, sd, ya, yb_hbm, z, h, wb, yb, hm,
                  pos_v, off_v, off_s, wsem, xsem, ysem, osem, usem):
    ne, d, ff = wg.shape
    members, tokens = x_hbm.shape[:2]
    nf, nd = ff // CW, d // CW
    gitems, ditems = nf * ne, nd * ne
    ring = 3
    f32, bf16, i32 = jnp.float32, jnp.bfloat16, jnp.int32

    def gcopy(i, slot):
        e, f = lax.rem(i, ne), lax.div(i, ne)
        c = pl.ds(pl.multiple_of(f * CW, CW), CW)
        return [
            pltpu.make_async_copy(w.at[e, :, c], wb.at[2 * slot + k], wsem.at[2 * slot + k])
            for k, w in enumerate((wg, wu))
        ]

    def dcopy(i, slot):
        e, f = lax.rem(i, ne), lax.div(i, ne)
        c = pl.ds(pl.multiple_of(f * CW, CW), CW)
        return [pltpu.make_async_copy(wd.at[e, :, c], wb.at[slot, pl.ds(0, ff)], wsem.at[slot])]

    def xcopy(s, b):
        return [
            pltpu.make_async_copy(x_hbm.at[s, :, pl.ds(c * CW, CW)], yb.at[b, c], xsem.at[b, c])
            for c in range(nd)
        ]

    def start(copies):
        for c in copies:
            c.start()

    def wait(copies):
        for c in copies:
            c.wait()

    start(xcopy(0, 0))
    start(xcopy(1, 1))
    start(gcopy(0, 0))

    rows = members * ne
    me = lax.axis_index("ep")
    w = jnp.concatenate([wt_ref[s, me] for s in range(members)], axis=0)
    mask = w != 0.0
    mb = jnp.where(mask, 1.0, 0.0).astype(bf16)
    a0 = lax.broadcasted_iota(i32, (tokens, tokens), 0)
    a1 = lax.broadcasted_iota(i32, (tokens, tokens), 1)
    rank = dot(mb, jnp.where(a0 <= a1, 1.0, 0.0).astype(bf16))
    b0 = lax.broadcasted_iota(i32, (rows, rows), 0)
    b1 = lax.broadcasted_iota(i32, (rows, rows), 1)
    earlier = (lax.rem(b0, ne) == lax.rem(b1, ne)) & (b1 < b0)
    before = jnp.sum(dot(jnp.where(earlier, 1.0, 0.0).astype(bf16), mb), axis=1, keepdims=True)
    count = jnp.sum(jnp.where(mask, 1.0, 0.0), axis=1, keepdims=True)
    pos = jnp.where(mask, before + rank - 1.0, -1.0)
    for s in range(members):
        pos_v[s, 0:ne, :] = pos[s * ne:(s + 1) * ne]
    lane = lax.broadcasted_iota(i32, (rows, 128), 1)
    total = jnp.zeros((rows, tokens), f32)
    for s in range(members):
        every = jnp.concatenate([wt_ref[s, m] for m in range(members)], axis=0)
        total += jnp.where(every != 0.0, 1.0, 0.0)
    total = jnp.sum(total, axis=1, keepdims=True)
    off_v[...] = jnp.where(lane == 0, before, jnp.where(lane == 1, before + count, total)).astype(i32)
    cp = pltpu.make_async_copy(off_v, off_s, osem)
    cp.start()
    zero = jnp.zeros((16, d), bf16)

    def clear(i, _):
        for e in range(ne):
            z[e, pl.ds(pl.multiple_of(i * 16, 16), 16), :] = zero
        return 0

    lax.fori_loop(0, z.shape[1] // 16, clear, 0)
    cp.wait()

    costs = []
    for m in range(members):
        c = 0
        for e in range(ne):
            c += lax.div(off_s[m * ne + e, 2] + 127, 128) * 128
        costs.append(jnp.maximum(c, LEAST_COST))

    def give(_, carry):
        cost, held = carry
        best, who = jnp.where(held[0] < UNITS, cost[0], 1 << 20), 0
        for m in range(1, members):
            c = jnp.where(held[m] < UNITS, cost[m], 1 << 20)
            who = jnp.where(c < best, m, who)
            best = jnp.minimum(c, best)
        return (
            [jnp.where(who == m, cost[m] + UNIT_COST, cost[m]) for m in range(members)],
            [jnp.where(who == m, held[m] + 1, held[m]) for m in range(members)],
        )

    _, held = lax.fori_loop(0, units, give, (costs, [jnp.int32(0)] * members))
    first_unit, mine = 0, 0
    for m in range(members):
        first_unit += jnp.where(m < me, held[m], 0)
        mine += jnp.where(m == me, held[m], 0)

    block0 = lax.div(first_unit, 2)
    blocks = jnp.where(mine > 0, lax.div(first_unit + mine + 1, 2) - block0, 0)

    def block_col(b):
        return pl.multiple_of(lo + (block0 + b) * UW, UW)

    def ucopy(b):
        return [
            pltpu.make_async_copy(
                w.at[:, pl.ds(block_col(b), UW)], wb.at[2 + b, :, pl.ds(k * UW, UW)], usem.at[b, k]
            )
            for k, w in enumerate((sg, su))
        ]

    def vcopy(b, q, par):
        c = pl.ds(pl.multiple_of(q * CW, CW), CW)
        return pltpu.make_async_copy(
            sd.at[pl.ds(block_col(b), UW), c],
            z.at[b, pl.ds(0, UW), pl.ds(pl.multiple_of((2 + par) * CW, CW), CW)],
            usem.at[b, par],
        )

    def for_blocks(fn):
        for b in range(BLOCKS):
            @pl.when(b < blocks)
            def _():
                fn(b)

    for_blocks(lambda b: start(ucopy(b)))

    def blocks_of(half):
        kind = lax.rem(half + me, 2)
        b0 = lax.div(first_unit - kind + 1, 2)
        return b0 - block0, lax.div(first_unit + mine - kind + 1, 2) - b0

    def window(s, e):
        st = off_s[s * ne + e, 0]
        return pl.multiple_of(lax.div(st, 16) * 16, 16)

    def cmat(s):
        row = pl.multiple_of(lax.rem(s, 2) * tokens, tokens) if not isinstance(s, int) else s % 2 * tokens
        at = lax.div(s, 2) if not isinstance(s, int) else s // 2
        return z.at[at, pl.ds(row, tokens), pl.ds(4 * CW, CW)]

    def cwindow(s, e):
        return pl.multiple_of(jnp.minimum(window(s, e), z.shape[1] - CWIN), 16)

    wl = lax.broadcasted_iota(i32, (WIN, tokens), 0)

    def dispatch(s, _):
        b = lax.rem(s, 2)
        wait(xcopy(s, b))
        w0 = [window(s, e) for e in range(ne)]
        oh = jnp.concatenate([
            jnp.where(pos_v[s, e:e + 1, :].astype(i32) - w0[e] == wl, 1.0, 0.0).astype(bf16)
            for e in range(ne)
        ], axis=0)
        for c in range(nd):
            got = dot(oh, yb[b, c]).astype(bf16)
            for e in range(ne):
                at = (e, pl.ds(w0[e], WIN), slice(c * CW, (c + 1) * CW))
                z[at] = z[at] + got[e * WIN:(e + 1) * WIN]

        @pl.when(s == 0)
        def _():
            for_blocks(lambda b: wait(ucopy(b)))

        b0, nb = blocks_of(lax.div(s, 4))

        def unit(k, _):
            gu = dot(yb[b, 0], wb[2 + b0 + k, 0:CW, :])
            for c in range(1, nd):
                gu += dot(yb[b, c], wb[2 + b0 + k, c * CW:(c + 1) * CW, :])
            hm[b0 + k, s] = silu_mul(gu[:, :UW], gu[:, UW:])
            return 0

        lax.fori_loop(0, nb, unit, 0)

        @pl.when(s + 2 < members)
        def _():
            start(xcopy(s + 2, b))

        return 0

    lax.fori_loop(0, members, dispatch, 0)
    for i in range(1, ring):
        start(gcopy(i, i))

    def tiles(e, body):
        n = off_s[(members - 1) * ne + e, 1]
        most = h.shape[1]
        full = jnp.where(n > 512, 0, lax.div(n + 127, 256))
        lax.fori_loop(0, full, lambda m, c: (body(pl.multiple_of(m * 256, 256), 256), c)[1], 0)

        @pl.when((n > full * 256) & (n <= 512))
        def _():
            body(pl.multiple_of(full * 256, 256), 128)

        @pl.when(n > 512)
        def _():
            body(0, most)

    def kdot(a, b, m, size, c, step, k):
        part = k // 2 if size > 256 else k
        o = None
        for j in range(0, k, part):
            one = dot(a[pl.ds(m, size), j:j + part], b[j:j + part, c:c + step])
            o = one if o is None else o + one
        return o

    def gstep(i, _):
        e, f = lax.rem(i, ne), lax.div(i, ne)
        slot = lax.rem(i, ring)
        wait(gcopy(i, slot))
        def body(m, size):
            step = 256 if size > 256 else CW
            for c in range(0, CW, step):
                g = kdot(z.at[e], wb.at[2 * slot], m, size, c, step, d)
                u = kdot(z.at[e], wb.at[2 * slot + 1], m, size, c, step, d)
                h[e, pl.ds(m, size), pl.ds(pl.multiple_of(f * CW + c, step), step)] = silu_mul(g, u)

        tiles(e, body)

        @pl.when(i + ring < gitems)
        def _():
            start(gcopy(i + ring, slot))

        @pl.when(i + ring >= gitems)
        def _():
            start(dcopy(2 * (i + ring - gitems), 2 * slot))
            start(dcopy(2 * (i + ring - gitems) + 1, 2 * slot + 1))

        return 0

    lax.fori_loop(0, gitems, gstep, 0)

    both = jnp.concatenate([pos, w, jnp.zeros((128 - 2 * rows, tokens), f32)], axis=0).T
    cl = lax.broadcasted_iota(i32, (tokens, CWIN), 1)
    for s in range(members):
        for e in range(ne):
            k = s * ne + e
            rel = both[:, k:k + 1].astype(i32) - cwindow(s, e)
            cmat(s)[:, e * CWIN:(e + 1) * CWIN] = jnp.where(
                rel == cl, both[:, rows + k:rows + k + 1], 0.0
            ).astype(bf16)

    def ycopy(q, par):
        c = pl.ds(pl.multiple_of(q * CW, CW), CW)
        half = members // 2
        return [
            pltpu.make_async_copy(yb.at[par, pl.ds(k * half, half)], y.at[:, :, c], ysem.at[par, k])
            for k, y in enumerate((ya, yb_hbm))
        ]

    for_blocks(lambda u: vcopy(u, 0, 0).start())

    def dpair(q, _):
        par = lax.rem(q, 2)

        @pl.when(q + 1 < nd)
        def _():
            for_blocks(lambda u: vcopy(u, q + 1, 1 - par).start())

        oc = pl.ds(pl.multiple_of(par * CW, CW), CW)

        def estep(e, _):
            i = q * ne + e
            slot = lax.rem(i + 2 * gitems, 2 * ring)
            wait(dcopy(i, slot))

            def body(m, size):
                step = 256 if size > 256 else CW
                for c in range(0, CW, step):
                    o = kdot(h.at[e], wb.at[slot], m, size, c, step, ff)
                    z[e, pl.ds(m, size), pl.ds(pl.multiple_of(par * CW + c, step), step)] = o.astype(bf16)

            tiles(e, body)

            @pl.when(i + 2 * ring < ditems)
            def _():
                start(dcopy(i + 2 * ring, slot))

            return 0

        lax.fori_loop(0, ne, estep, 0)

        @pl.when(q >= 2)
        def _():
            wait(ycopy(q - 2, par))

        for_blocks(lambda u: vcopy(u, q, par).wait())
        vc = pl.ds(pl.multiple_of((2 + par) * CW, CW), CW)

        def two(k, _):
            b0, nb = blocks_of(lax.div(k, 2))
            for n in range(BLOCKS + 1):
                @pl.when(nb == n)
                def _():
                    for j in range(2):
                        s = 2 * k + j
                        o = None
                        for e in range(0, ne, 2):
                            rows2 = [z[e + i, pl.ds(cwindow(s, e + i), CWIN), oc] for i in range(2)]
                            one = dot(cmat(s)[:, e * CWIN:(e + 2) * CWIN], jnp.concatenate(rows2, axis=0))
                            o = one if o is None else o + one
                        for i in range(n):
                            o += dot(hm[b0 + i, s], z[b0 + i, 0:UW, vc])
                        yb[par, s] = o.astype(bf16)
            return 0

        lax.fori_loop(0, members // 2, two, 0)
        start(ycopy(q, par))
        return 0

    lax.fori_loop(0, nd, dpair, 0)
    wait(ycopy(nd - 2, (nd - 2) % 2))
    wait(ycopy(nd - 1, (nd - 1) % 2))


def routed(x_all, wt, wg, wu, wd, sg, su, sd, lo, width):
    members, tokens, d = x_all.shape
    ne, _, ff = wg.shape
    rows = members * 80
    anyspec = pl.BlockSpec(memory_space=pl.ANY)
    vspec = pl.BlockSpec(memory_space=pltpu.VMEM)
    half = jax.ShapeDtypeStruct((members // 2, tokens, d), jnp.bfloat16)
    return pl.pallas_call(
        functools.partial(routed_kernel, lo, 2 * width // UW),
        out_shape=(half, half),
        in_specs=[anyspec, vspec] + [anyspec] * 6,
        out_specs=(anyspec, anyspec),
        scratch_shapes=[
            pltpu.VMEM((ne, rows + 16, d), jnp.bfloat16),
            pltpu.VMEM((ne, rows, ff), jnp.bfloat16),
            pltpu.VMEM((6, d, CW), jnp.bfloat16),
            pltpu.VMEM((2, members, tokens, CW), jnp.bfloat16),
            pltpu.VMEM((BLOCKS, members, tokens, UW), jnp.bfloat16),
            pltpu.VMEM((members, 8, tokens), jnp.float32),
            pltpu.VMEM((members * ne, 128), jnp.int32),
            pltpu.SMEM((members * ne, 128), jnp.int32),
            pltpu.SemaphoreType.DMA((6,)),
            pltpu.SemaphoreType.DMA((2, d // CW)),
            pltpu.SemaphoreType.DMA((2, 2)),
            pltpu.SemaphoreType.DMA,
            pltpu.SemaphoreType.DMA((BLOCKS, 2)),
        ],
        compiler_params=pltpu.CompilerParams(vmem_limit_bytes=VMEM),
        cost_estimate=pl.CostEstimate(
            flops=6 * 1600 * d * ff, bytes_accessed=6 * ne * d * ff, transcendentals=1600 * ff
        ),
        name="routed",
    )(x_all, wt, wg, wu, wd, sg, su, sd)


def solution(mesh):
    members = mesh.shape["ep"]

    def body(x, expert, slot, gate, wg, wu, wd, sg, su, sd):
        tokens, top = expert.shape[2:]
        experts = wg.shape[0] * members
        slots = 5 * tokens * top // (4 * experts)
        middle = sg.shape[1] - 2 * EDGE * CW
        x2 = x.reshape(tokens, x.shape[-1])
        f32, bf16 = jnp.float32, jnp.bfloat16

        g = jnp.where(slot < slots, gate.astype(bf16).astype(f32), 0.0).reshape(tokens, top)
        ids = expert.reshape(tokens, top)
        dense = jnp.sum(
            jnp.where(ids.T[:, None, :] == jnp.arange(experts)[None, :, None], g.T[:, None, :], 0.0), axis=0
        ).reshape(members, -1, tokens)
        acc, x_all, w_all = first(x2, dense, sg, su, sd, 0, EDGE)
        ya, yb = routed(x_all, w_all, wg, wu, wd, sg, su, sd, EDGE * CW, middle)
        y = last(x2, ya, yb, acc, sg, su, sd, EDGE * CW + middle, EDGE)
        return y.reshape(x.shape)

    a = P("dp", "ep", None, None)
    w = P("ep", None, None)
    s = P(None, None)
    return jax.shard_map(
        body, mesh=mesh, in_specs=(a, a, a, a, w, w, w, s, s, s), out_specs=a, check_vma=False
    )
```

```python
import functools

import jax
import jax.numpy as jnp
from jax import lax
from jax.experimental import pallas as pl
from jax.experimental.pallas import tpu as pltpu
from jax.sharding import PartitionSpec as P

CW = 512
WIN = 96
CWIN = 128
VMEM = 67_043_328


def silu_mul(g, u):
    return (g * jax.nn.sigmoid(g) * u).astype(jnp.bfloat16)


def dot(a, b):
    return jnp.dot(a, b, preferred_element_type=jnp.float32)


FLIPS = ((0, 0, 0), (0, 1, 0), (1, 0, 0), (1, 1, 0), (0, 0, 1), (0, 1, 1), (1, 0, 1), (1, 1, 1))
CHUNKS = 4
EDGE = 18
HALVES = 6
ROWS = 3072


def member(flip):
    me = lax.axis_index("ep")
    x, y, c = lax.div(me, 4), lax.rem(lax.div(me, 2), 2), lax.rem(me, 2)
    fx, fy, fc = flip
    return (x + fx * (1 - 2 * x)) * 4 + (y + fy * (1 - 2 * y)) * 2 + c + fc * (1 - 2 * c)


def greet():
    barrier = pltpu.get_barrier_semaphore()
    for flip in FLIPS[1:]:
        pl.semaphore_signal(
            barrier, inc=1, device_id={"ep": member(flip)}, device_id_type=pl.DeviceIdType.MESH
        )
    pl.semaphore_wait(barrier, len(FLIPS) - 1)


def remote(src, dst, ssem, rsem, to):
    return pltpu.make_async_remote_copy(
        src_ref=src, dst_ref=dst, send_sem=ssem, recv_sem=rsem,
        device_id={"ep": to}, device_id_type=pl.DeviceIdType.MESH,
    )


def start_all(copies):
    for c in copies:
        c.start()


def wait_all(copies):
    for c in copies:
        c.wait()


class Shared:
    def __init__(self, lo, tiles, x, sg, su, sd, h, wb, wsem):
        self.lo, self.tiles, self.nd = lo, tiles, x.shape[1] // CW
        self.x, self.sg, self.su, self.sd, self.h, self.wb, self.wsem = x, sg, su, sd, h, wb, wsem
        self.parts = tiles * CW // ROWS

    def up(self, i, slot):
        c = pl.ds(pl.multiple_of(self.lo + i * CW, CW), CW)
        return [
            pltpu.make_async_copy(w.at[:, c], self.wb.at[2 * slot + k], self.wsem.at[2 * slot + k])
            for k, w in enumerate((self.sg, self.su))
        ]

    def down(self, j, r, slot):
        c = pl.ds(pl.multiple_of(j * CW, CW), CW)
        return pltpu.make_async_copy(
            self.sd.at[pl.ds(self.lo + r * ROWS, ROWS), c], self.wb.at[slot, pl.ds(0, ROWS)], self.wsem.at[slot]
        )

    def begin(self):
        for i in range(HALVES // 2):
            start_all(self.up(i, i))

    def run(self, store, up_hooks, down_hooks):
        ring, tiles, nd, parts, h, wb = HALVES // 2, self.tiles, self.nd, self.parts, self.h, self.wb

        def up(i, _):
            slot = lax.rem(i, ring)
            wait_all(self.up(i, slot))
            g = dot(self.x[...], wb[2 * slot])
            u = dot(self.x[...], wb[2 * slot + 1])
            h[:, pl.ds(pl.multiple_of(i * CW, CW), CW)] = silu_mul(g, u)

            @pl.when(i + ring < tiles)
            def _():
                start_all(self.up(i + ring, slot))

            for k in range(ring):
                @pl.when(i == tiles - ring + k)
                def _():
                    for n in (2 * k, 2 * k + 1):
                        self.down(n // parts, n % parts, n).start()

            for at, fn in up_hooks:
                pl.when(i == at)(fn)
            return 0

        lax.fori_loop(0, tiles, up, 0)
        deep = HALVES // parts

        def down(j, _):
            base = lax.rem(j, deep) * parts
            o = None
            for r in range(parts):
                self.down(j, r, base + r).wait()
                d = dot(h[:, r * ROWS:(r + 1) * ROWS], wb[base + r, 0:ROWS, :])
                o = d if o is None else o + d
            store(pl.ds(pl.multiple_of(j * CW, CW), CW), o)

            @pl.when(j + deep < nd)
            def _():
                for r in range(parts):
                    self.down(j + deep, r, base + r).start()

            for at, fn in down_hooks:
                pl.when(j == at)(fn)
            return 0

        lax.fori_loop(0, nd, down, 0)


def first_kernel(lo, tiles, x, dense, sg, su, sd, out, x_all, w_all, h, wb, wsem, lsem, ssem, rsem, sw, rw):
    tokens = x.shape[0]
    core = lax.rem(lax.axis_index("ep"), 2)
    size = tokens // CHUNKS
    part = lambda k: pl.ds(k * size, size)
    work = Shared(lo, tiles, x, sg, su, sd, h, wb, wsem)
    work.begin()
    keep = [
        pltpu.make_async_copy(x, x_all.at[0], lsem.at[0]),
        pltpu.make_async_copy(dense, w_all.at[0], lsem.at[1]),
    ]
    start_all(keep)
    greet()

    own = lambda p, k: remote(
        x.at[part(k)], x_all.at[p, part(k)], ssem.at[p, k], rsem.at[p, k], member(FLIPS[p])
    )
    diag_to = (1 - core) * member(FLIPS[1]) + core * member(FLIPS[2])
    diag = lambda k: remote(
        x_all.at[2 - core, part(k)], x_all.at[3, part(k)], ssem.at[3, k], rsem.at[3, k], diag_to
    )
    mate = lambda p, k: remote(
        x_all.at[p, part(k)], x_all.at[p + 4, part(k)], ssem.at[p + 4, k], rsem.at[p + 4, k], member(FLIPS[4])
    )
    small = [
        remote(dense, w_all.at[p], sw.at[p], rw.at[p], member(FLIPS[p])) for p in range(1, len(FLIPS))
    ]
    start_all(small)
    for k in range(CHUNKS):
        own(1, k).start()
        own(2, k).start()
    for k in range(CHUNKS):
        own(4, k).start()

    def arrived(k):
        own(1, k).wait_recv()
        own(2, k).wait_recv()
        diag(k).start()
        mate(1, k).start()
        mate(2, k).start()

    def around(k):
        diag(k).wait_recv()
        mate(3, k).start()

    up_hooks = [(6, lambda: arrived(0)), (10, lambda: arrived(1)), (14, lambda: arrived(2))]
    down_hooks = [
        (0, lambda: arrived(3)), (2, lambda: around(0)), (4, lambda: around(1)), (5, lambda: around(2)), (6, lambda: around(3)),
    ]

    def store(c, o):
        out[:, c] = o

    work.run(store, up_hooks, down_hooks)
    wait_all(keep)
    wait_all(small)
    for k in range(CHUNKS):
        own(1, k).wait_send()
        own(2, k).wait_send()
        diag(k).wait_send()
        own(4, k).wait()
        for p in (1, 2, 3):
            mate(p, k).wait()


def last_kernel(lo, tiles, x, ya, yb, base, sg, su, sd, out, h, wb, acc, tv, rb, dg, rxy,
                wsem, lsem, ysem, ssem, rsem, s2, r2):
    tokens, d = x.shape
    f32, bf16 = jnp.float32, jnp.bfloat16
    core = lax.rem(lax.axis_index("ep"), 2)
    size = tokens // CHUNKS
    part = lambda k: pl.ds(k * size, size)
    work = Shared(lo, tiles, x, sg, su, sd, h, wb, wsem)
    order = (3, 1, 2, 0)
    load = lambda p, k: pltpu.make_async_copy(ya.at[p, part(k)], tv.at[p, part(k)], ysem.at[p, k])
    for k in range(CHUNKS):
        load(3, k).start()
    work.begin()
    for p in order[1:]:
        for k in range(CHUNKS):
            load(p, k).start()
    basecopy = pltpu.make_async_copy(base, acc, lsem.at[0])
    basecopy.start()
    greet()

    swap = lambda p, k: remote(
        yb.at[p, part(k)], rb.at[p, part(k)], ssem.at[p, k], rsem.at[p, k], member(FLIPS[4])
    )
    for p in order:
        for k in range(CHUNKS):
            swap(p, k).start()

    to_y, to_x = member(FLIPS[1]), member(FLIPS[2])
    near = (1 - core) * to_x + core * to_y
    relay = (1 - core) * to_y + core * to_x
    direct, turned = 2 - core, 1 + core
    send0 = lambda k: remote(tv.at[3, part(k)], dg.at[part(k)], s2.at[0, k], r2.at[0, k], near)
    send1 = lambda k: remote(
        tv.at[direct, part(k)], rxy.at[direct - 1, part(k)], s2.at[direct, k], r2.at[direct, k], near
    )
    send2 = lambda k: remote(
        tv.at[turned, part(k)], rxy.at[turned - 1, part(k)], s2.at[turned, k], r2.at[turned, k], relay
    )

    def far(k):
        load(3, k).wait()
        swap(3, k).wait_recv()
        tv[3, part(k)] = (tv[3, part(k)].astype(f32) + rb[3, part(k)].astype(f32)).astype(bf16)
        send0(k).start()

    def straight(k):
        load(direct, k).wait()
        swap(direct, k).wait_recv()
        tv[direct, part(k)] = (tv[direct, part(k)].astype(f32) + rb[direct, part(k)].astype(f32)).astype(bf16)
        send1(k).start()

    def passed(k):
        load(turned, k).wait()
        swap(turned, k).wait_recv()
        send0(k).wait_recv()
        tv[turned, part(k)] = (
            tv[turned, part(k)].astype(f32) + rb[turned, part(k)].astype(f32) + dg[part(k)].astype(f32)
        ).astype(bf16)
        send2(k).start()

    def both(fn, *ks):
        def run():
            for k in ks:
                fn(k)
        return run

    both(far, 0, 1, 2, 3)()
    up_hooks = [
        (0, both(straight, 0, 1, 2, 3)), (3, both(passed, 0)), (5, both(passed, 1)), (7, both(passed, 2)),
        (9, both(passed, 3)), (11, basecopy.wait),
    ]

    def store(c, o):
        acc[:, c] = acc[:, c] + o

    work.run(store, up_hooks, [])
    for k in range(CHUNKS):
        load(0, k).wait()
        swap(0, k).wait_recv()
        for q in (1, 2):
            remote(tv.at[q, part(k)], rxy.at[q - 1, part(k)], s2.at[q, k], r2.at[q, k], to_y).wait_recv()

        def rows(i, _, k=k):
            r = pl.ds(pl.multiple_of(k * size + i * 16, 16), 16)
            out[r, :] = (
                acc[r, :] + tv[0, r, :].astype(f32) + rb[0, r, :].astype(f32)
                + rxy[0, r, :].astype(f32) + rxy[1, r, :].astype(f32)
            ).astype(bf16)
            return 0

        lax.fori_loop(0, size // 16, rows, 0)
    for k in range(CHUNKS):
        for p in range(4):
            swap(p, k).wait_send()
        send0(k).wait_send()
        send1(k).wait_send()
        send2(k).wait_send()


ANY = pl.BlockSpec(memory_space=pl.ANY)
VM = pl.BlockSpec(memory_space=pltpu.VMEM)


def shared_cost(tokens, d, width):
    return pl.CostEstimate(
        flops=6 * tokens * d * width, bytes_accessed=6 * d * width, transcendentals=tokens * width
    )


def first(x, dense, sg, su, sd, lo, tiles):
    tokens, d = x.shape
    n = len(FLIPS)
    dma = pltpu.SemaphoreType.DMA
    return pl.pallas_call(
        functools.partial(first_kernel, lo, tiles),
        out_shape=(
            jax.ShapeDtypeStruct((tokens, d), jnp.float32),
            jax.ShapeDtypeStruct((n, tokens, d), x.dtype),
            jax.ShapeDtypeStruct((n, *dense.shape), dense.dtype),
        ),
        in_specs=[VM, VM, ANY, ANY, ANY],
        out_specs=(VM, ANY, ANY),
        scratch_shapes=[
            pltpu.VMEM((tokens, tiles * CW), jnp.bfloat16),
            pltpu.VMEM((HALVES, d, CW), jnp.bfloat16),
            dma((HALVES,)), dma((2,)), dma((n, CHUNKS)), dma((n, CHUNKS)), dma((n,)), dma((n,)),
        ],
        compiler_params=pltpu.CompilerParams(vmem_limit_bytes=VMEM, collective_id=0, has_side_effects=True),
        cost_estimate=shared_cost(tokens, d, tiles * CW),
        name="first",
    )(x, dense, sg, su, sd)


def last(x, ya, yb, base, sg, su, sd, lo, tiles):
    tokens, d = x.shape
    dma = pltpu.SemaphoreType.DMA
    bf16 = jnp.bfloat16
    return pl.pallas_call(
        functools.partial(last_kernel, lo, tiles),
        out_shape=jax.ShapeDtypeStruct((tokens, d), bf16),
        in_specs=[VM, ANY, ANY, ANY, ANY, ANY, ANY],
        out_specs=VM,
        scratch_shapes=[
            pltpu.VMEM((tokens, tiles * CW), bf16),
            pltpu.VMEM((HALVES, d, CW), bf16),
            pltpu.VMEM((tokens, d), jnp.float32),
            pltpu.VMEM((4, tokens, d), bf16),
            pltpu.VMEM((4, tokens, d), bf16),
            pltpu.VMEM((tokens, d), bf16),
            pltpu.VMEM((2, tokens, d), bf16),
            dma((HALVES,)), dma((1,)), dma((4, CHUNKS)), dma((4, CHUNKS)), dma((4, CHUNKS)),
            dma((3, CHUNKS)), dma((3, CHUNKS)),
        ],
        compiler_params=pltpu.CompilerParams(vmem_limit_bytes=VMEM, collective_id=1, has_side_effects=True),
        cost_estimate=shared_cost(tokens, d, tiles * CW),
        name="last",
    )(x, ya, yb, base, sg, su, sd)


UNITS = 5
BLOCKS = 3
UW = 256
UNIT_COST = 140
LEAST_COST = 880


def routed_kernel(lo, units, x_hbm, wt_ref, wg, wu, wd, sg, su, sd, ya, yb_hbm, z, h, wb, yb, hm,
                  pos_v, off_v, off_s, wsem, xsem, ysem, osem, usem):
    ne, d, ff = wg.shape
    members, tokens = x_hbm.shape[:2]
    nf, nd = ff // CW, d // CW
    gitems, ditems = nf * ne, nd * ne
    ring = 3
    f32, bf16, i32 = jnp.float32, jnp.bfloat16, jnp.int32

    def gcopy(i, slot):
        e, f = lax.rem(i, ne), lax.div(i, ne)
        c = pl.ds(pl.multiple_of(f * CW, CW), CW)
        return [
            pltpu.make_async_copy(w.at[e, :, c], wb.at[2 * slot + k], wsem.at[2 * slot + k])
            for k, w in enumerate((wg, wu))
        ]

    def dcopy(i, slot):
        e, f = lax.rem(i, ne), lax.div(i, ne)
        c = pl.ds(pl.multiple_of(f * CW, CW), CW)
        return [pltpu.make_async_copy(wd.at[e, :, c], wb.at[slot, pl.ds(0, ff)], wsem.at[slot])]

    def xcopy(s, b):
        return [
            pltpu.make_async_copy(x_hbm.at[s, :, pl.ds(c * CW, CW)], yb.at[b, c], xsem.at[b, c])
            for c in range(nd)
        ]

    def start(copies):
        for c in copies:
            c.start()

    def wait(copies):
        for c in copies:
            c.wait()

    start(xcopy(0, 0))
    start(xcopy(1, 1))
    start(gcopy(0, 0))

    rows = members * ne
    me = lax.axis_index("ep")
    w = jnp.concatenate([wt_ref[s, me] for s in range(members)], axis=0)
    mask = w != 0.0
    mb = jnp.where(mask, 1.0, 0.0).astype(bf16)
    a0 = lax.broadcasted_iota(i32, (tokens, tokens), 0)
    a1 = lax.broadcasted_iota(i32, (tokens, tokens), 1)
    rank = dot(mb, jnp.where(a0 <= a1, 1.0, 0.0).astype(bf16))
    b0 = lax.broadcasted_iota(i32, (rows, rows), 0)
    b1 = lax.broadcasted_iota(i32, (rows, rows), 1)
    earlier = (lax.rem(b0, ne) == lax.rem(b1, ne)) & (b1 < b0)
    before = jnp.sum(dot(jnp.where(earlier, 1.0, 0.0).astype(bf16), mb), axis=1, keepdims=True)
    count = jnp.sum(jnp.where(mask, 1.0, 0.0), axis=1, keepdims=True)
    pos = jnp.where(mask, before + rank - 1.0, -1.0)
    for s in range(members):
        pos_v[s, 0:ne, :] = pos[s * ne:(s + 1) * ne]
    lane = lax.broadcasted_iota(i32, (rows, 128), 1)
    total = jnp.zeros((rows, tokens), f32)
    for s in range(members):
        every = jnp.concatenate([wt_ref[s, m] for m in range(members)], axis=0)
        total += jnp.where(every != 0.0, 1.0, 0.0)
    total = jnp.sum(total, axis=1, keepdims=True)
    off_v[...] = jnp.where(lane == 0, before, jnp.where(lane == 1, before + count, total)).astype(i32)
    cp = pltpu.make_async_copy(off_v, off_s, osem)
    cp.start()
    zero = jnp.zeros((16, d), bf16)

    def clear(i, _):
        for e in range(ne):
            z[e, pl.ds(pl.multiple_of(i * 16, 16), 16), :] = zero
        return 0

    lax.fori_loop(0, z.shape[1] // 16, clear, 0)
    cp.wait()

    costs = []
    for m in range(members):
        c = 0
        for e in range(ne):
            c += lax.div(off_s[m * ne + e, 2] + 127, 128) * 128
        costs.append(jnp.maximum(c, LEAST_COST))

    def give(_, carry):
        cost, held = carry
        best, who = jnp.where(held[0] < UNITS, cost[0], 1 << 20), 0
        for m in range(1, members):
            c = jnp.where(held[m] < UNITS, cost[m], 1 << 20)
            who = jnp.where(c < best, m, who)
            best = jnp.minimum(c, best)
        return (
            [jnp.where(who == m, cost[m] + UNIT_COST, cost[m]) for m in range(members)],
            [jnp.where(who == m, held[m] + 1, held[m]) for m in range(members)],
        )

    _, held = lax.fori_loop(0, units, give, (costs, [jnp.int32(0)] * members))
    first_unit, mine = 0, 0
    for m in range(members):
        first_unit += jnp.where(m < me, held[m], 0)
        mine += jnp.where(m == me, held[m], 0)

    block0 = lax.div(first_unit, 2)
    blocks = jnp.where(mine > 0, lax.div(first_unit + mine + 1, 2) - block0, 0)

    def block_col(b):
        return pl.multiple_of(lo + (block0 + b) * UW, UW)

    def ucopy(b):
        return [
            pltpu.make_async_copy(
                w.at[:, pl.ds(block_col(b), UW)], wb.at[2 + b, :, pl.ds(k * UW, UW)], usem.at[b, k]
            )
            for k, w in enumerate((sg, su))
        ]

    def vcopy(b, q, par):
        c = pl.ds(pl.multiple_of(q * CW, CW), CW)
        return pltpu.make_async_copy(
            sd.at[pl.ds(block_col(b), UW), c],
            z.at[b, pl.ds(0, UW), pl.ds(pl.multiple_of((2 + par) * CW, CW), CW)],
            usem.at[b, par],
        )

    def for_blocks(fn):
        for b in range(BLOCKS):
            @pl.when(b < blocks)
            def _():
                fn(b)

    for_blocks(lambda b: start(ucopy(b)))

    def blocks_of(half):
        kind = lax.rem(half + me, 2)
        b0 = lax.div(first_unit - kind + 1, 2)
        return b0 - block0, lax.div(first_unit + mine - kind + 1, 2) - b0

    def window(s, e):
        st = off_s[s * ne + e, 0]
        return pl.multiple_of(lax.div(st, 16) * 16, 16)

    def cmat(s):
        row = pl.multiple_of(lax.rem(s, 2) * tokens, tokens) if not isinstance(s, int) else s % 2 * tokens
        at = lax.div(s, 2) if not isinstance(s, int) else s // 2
        return z.at[at, pl.ds(row, tokens), pl.ds(4 * CW, CW)]

    def cwindow(s, e):
        return pl.multiple_of(jnp.minimum(window(s, e), z.shape[1] - CWIN), 16)

    wl = lax.broadcasted_iota(i32, (WIN, tokens), 0)

    def dispatch(s, _):
        b = lax.rem(s, 2)
        wait(xcopy(s, b))
        w0 = [window(s, e) for e in range(ne)]
        oh = jnp.concatenate([
            jnp.where(pos_v[s, e:e + 1, :].astype(i32) - w0[e] == wl, 1.0, 0.0).astype(bf16)
            for e in range(ne)
        ], axis=0)
        for c in range(nd):
            got = dot(oh, yb[b, c]).astype(bf16)
            for e in range(ne):
                at = (e, pl.ds(w0[e], WIN), slice(c * CW, (c + 1) * CW))
                z[at] = z[at] + got[e * WIN:(e + 1) * WIN]

        @pl.when(s == 0)
        def _():
            for_blocks(lambda b: wait(ucopy(b)))

        b0, nb = blocks_of(lax.div(s, 4))

        def unit(k, _):
            gu = dot(yb[b, 0], wb[2 + b0 + k, 0:CW, :])
            for c in range(1, nd):
                gu += dot(yb[b, c], wb[2 + b0 + k, c * CW:(c + 1) * CW, :])
            hm[b0 + k, s] = silu_mul(gu[:, :UW], gu[:, UW:])
            return 0

        lax.fori_loop(0, nb, unit, 0)

        @pl.when(s + 2 < members)
        def _():
            start(xcopy(s + 2, b))

        return 0

    lax.fori_loop(0, members, dispatch, 0)
    for i in range(1, ring):
        start(gcopy(i, i))

    def tiles(e, body):
        n = off_s[(members - 1) * ne + e, 1]
        most = h.shape[1]
        full = jnp.where(n > 512, 0, lax.div(n + 127, 256))
        lax.fori_loop(0, full, lambda m, c: (body(pl.multiple_of(m * 256, 256), 256), c)[1], 0)

        @pl.when((n > full * 256) & (n <= 512))
        def _():
            body(pl.multiple_of(full * 256, 256), 128)

        @pl.when(n > 512)
        def _():
            body(0, most)

    def kdot(a, b, m, size, c, step, k):
        part = k // 2 if size > 256 else k
        o = None
        for j in range(0, k, part):
            one = dot(a[pl.ds(m, size), j:j + part], b[j:j + part, c:c + step])
            o = one if o is None else o + one
        return o

    def gstep(i, _):
        e, f = lax.rem(i, ne), lax.div(i, ne)
        slot = lax.rem(i, ring)
        wait(gcopy(i, slot))
        def body(m, size):
            step = 256 if size > 256 else CW
            for c in range(0, CW, step):
                g = kdot(z.at[e], wb.at[2 * slot], m, size, c, step, d)
                u = kdot(z.at[e], wb.at[2 * slot + 1], m, size, c, step, d)
                h[e, pl.ds(m, size), pl.ds(pl.multiple_of(f * CW + c, step), step)] = silu_mul(g, u)

        tiles(e, body)

        @pl.when(i + ring < gitems)
        def _():
            start(gcopy(i + ring, slot))

        @pl.when(i + ring >= gitems)
        def _():
            start(dcopy(2 * (i + ring - gitems), 2 * slot))
            start(dcopy(2 * (i + ring - gitems) + 1, 2 * slot + 1))

        return 0

    lax.fori_loop(0, gitems, gstep, 0)

    both = jnp.concatenate([pos, w, jnp.zeros((128 - 2 * rows, tokens), f32)], axis=0).T
    cl = lax.broadcasted_iota(i32, (tokens, CWIN), 1)
    for s in range(members):
        for e in range(ne):
            k = s * ne + e
            rel = both[:, k:k + 1].astype(i32) - cwindow(s, e)
            cmat(s)[:, e * CWIN:(e + 1) * CWIN] = jnp.where(
                rel == cl, both[:, rows + k:rows + k + 1], 0.0
            ).astype(bf16)

    def ycopy(q, par):
        c = pl.ds(pl.multiple_of(q * CW, CW), CW)
        half = members // 2
        return [
            pltpu.make_async_copy(yb.at[par, pl.ds(k * half, half)], y.at[:, :, c], ysem.at[par, k])
            for k, y in enumerate((ya, yb_hbm))
        ]

    for_blocks(lambda u: vcopy(u, 0, 0).start())

    def dpair(q, _):
        par = lax.rem(q, 2)

        @pl.when(q + 1 < nd)
        def _():
            for_blocks(lambda u: vcopy(u, q + 1, 1 - par).start())

        oc = pl.ds(pl.multiple_of(par * CW, CW), CW)

        def estep(e, _):
            i = q * ne + e
            slot = lax.rem(i + 2 * gitems, 2 * ring)
            wait(dcopy(i, slot))

            def body(m, size):
                step = 256 if size > 256 else CW
                for c in range(0, CW, step):
                    o = kdot(h.at[e], wb.at[slot], m, size, c, step, ff)
                    z[e, pl.ds(m, size), pl.ds(pl.multiple_of(par * CW + c, step), step)] = o.astype(bf16)

            tiles(e, body)

            @pl.when(i + 2 * ring < ditems)
            def _():
                start(dcopy(i + 2 * ring, slot))

            return 0

        lax.fori_loop(0, ne, estep, 0)

        @pl.when(q >= 2)
        def _():
            wait(ycopy(q - 2, par))

        for_blocks(lambda u: vcopy(u, q, par).wait())
        vc = pl.ds(pl.multiple_of((2 + par) * CW, CW), CW)

        def two(k, _):
            b0, nb = blocks_of(lax.div(k, 2))
            for n in range(BLOCKS + 1):
                @pl.when(nb == n)
                def _():
                    for j in range(2):
                        s = 2 * k + j
                        o = None
                        for e in range(0, ne, 2):
                            rows2 = [z[e + i, pl.ds(cwindow(s, e + i), CWIN), oc] for i in range(2)]
                            one = dot(cmat(s)[:, e * CWIN:(e + 2) * CWIN], jnp.concatenate(rows2, axis=0))
                            o = one if o is None else o + one
                        for i in range(n):
                            o += dot(hm[b0 + i, s], z[b0 + i, 0:UW, vc])
                        yb[par, s] = o.astype(bf16)
            return 0

        lax.fori_loop(0, members // 2, two, 0)
        start(ycopy(q, par))
        return 0

    lax.fori_loop(0, nd, dpair, 0)
    wait(ycopy(nd - 2, (nd - 2) % 2))
    wait(ycopy(nd - 1, (nd - 1) % 2))


def routed(x_all, wt, wg, wu, wd, sg, su, sd, lo, width):
    members, tokens, d = x_all.shape
    ne, _, ff = wg.shape
    rows = members * 80
    anyspec = pl.BlockSpec(memory_space=pl.ANY)
    vspec = pl.BlockSpec(memory_space=pltpu.VMEM)
    half = jax.ShapeDtypeStruct((members // 2, tokens, d), jnp.bfloat16)
    return pl.pallas_call(
        functools.partial(routed_kernel, lo, 2 * width // UW),
        out_shape=(half, half),
        in_specs=[anyspec, vspec] + [anyspec] * 6,
        out_specs=(anyspec, anyspec),
        scratch_shapes=[
            pltpu.VMEM((ne, rows + 16, d), jnp.bfloat16),
            pltpu.VMEM((ne, rows, ff), jnp.bfloat16),
            pltpu.VMEM((6, d, CW), jnp.bfloat16),
            pltpu.VMEM((2, members, tokens, CW), jnp.bfloat16),
            pltpu.VMEM((BLOCKS, members, tokens, UW), jnp.bfloat16),
            pltpu.VMEM((members, 8, tokens), jnp.float32),
            pltpu.VMEM((members * ne, 128), jnp.int32),
            pltpu.SMEM((members * ne, 128), jnp.int32),
            pltpu.SemaphoreType.DMA((6,)),
            pltpu.SemaphoreType.DMA((2, d // CW)),
            pltpu.SemaphoreType.DMA((2, 2)),
            pltpu.SemaphoreType.DMA,
            pltpu.SemaphoreType.DMA((BLOCKS, 2)),
        ],
        compiler_params=pltpu.CompilerParams(vmem_limit_bytes=VMEM),
        cost_estimate=pl.CostEstimate(
            flops=6 * 1600 * d * ff, bytes_accessed=6 * ne * d * ff, transcendentals=1600 * ff
        ),
        name="routed",
    )(x_all, wt, wg, wu, wd, sg, su, sd)


def solution(mesh):
    members = mesh.shape["ep"]

    def body(x, expert, slot, gate, wg, wu, wd, sg, su, sd):
        tokens, top = expert.shape[2:]
        experts = wg.shape[0] * members
        slots = 5 * tokens * top // (4 * experts)
        middle = sg.shape[1] - 2 * EDGE * CW
        x2 = x.reshape(tokens, x.shape[-1])
        f32, bf16 = jnp.float32, jnp.bfloat16

        g = jnp.where(slot < slots, gate.astype(bf16).astype(f32), 0.0).reshape(tokens, top)
        ids = expert.reshape(tokens, top)
        dense = jnp.sum(
            jnp.where(ids.T[:, None, :] == jnp.arange(experts)[None, :, None], g.T[:, None, :], 0.0), axis=0
        ).reshape(members, -1, tokens)
        acc, x_all, w_all = first(x2, dense, sg, su, sd, 0, EDGE)
        ya, yb = routed(x_all, w_all, wg, wu, wd, sg, su, sd, EDGE * CW, middle)
        y = last(x2, ya, yb, acc, sg, su, sd, EDGE * CW + middle, EDGE)
        return y.reshape(x.shape)

    a = P("dp", "ep", None, None)
    w = P("ep", None, None)
    s = P(None, None)
    return jax.shard_map(
        body, mesh=mesh, in_specs=(a, a, a, a, w, w, w, s, s, s), out_specs=a, check_vma=False
    )
```
